32 devices in a mesh: row: 4 (over y, x), col: 8 (over z, core).
Axes of the slice: x: 2, y: 2, z: 4, core: 2. Of those that a mesh axis runs over, the one named last changes fastest.
Arguments:
- inverse_factor: bfloat16 [8192, 8192], P('row', 'col'), may hold values from -1 to 2, as said below
- alpha_vector: float32 [8192], replicated, may hold values from -2 to 2
Outputs:
- weight_matrix: float32 [8192, 8192], P(('row', 'col'))
The draws below stay inside these ranges and needn't reach their ends.
Inputs may be any that keep to these rules, and one draw needn't show every extreme that they name: `inverse_factor`: lower triangular: every entry above the diagonal is zero; diagonal entries lie between 1 and 2.
All inputs are finite; a program needn't handle non-finite values.
Results may differ from the reference program's by a relative error of at most 0.0003.
Values may be sent and summed in bfloat16 or wider, within the bound.
A program may use at most 128 MiB of HBM per device.

```python
import jax
import jax.numpy as jnp

N = 8192


def draw_inverse_factor(key, part):
    first = jax.random.fold_in(key, 11)
    second = jax.random.fold_in(key, 23)
    spread = jnp.clip(jax.random.normal(first, (N, N), jnp.float32), -6.0, 6.0)
    diagonal = jnp.exp(jax.random.uniform(second, (N,), jnp.float32, 0.0, 0.6931472))
    lower = jnp.tril(spread * (2.0 / jnp.sqrt(jnp.float32(N))), -1)
    return (lower + jnp.diag(diagonal)).astype(jnp.bfloat16)


def bell_draw(key, dims, scale, bound, held_as=jnp.bfloat16):
    drawn = jax.random.normal(key, dims, jnp.float32) * scale
    return jnp.minimum(jnp.maximum(drawn, -bound), bound).astype(held_as)


def setup_inputs(seed: int = 0) -> dict:
    key_list = jax.random.split(jax.random.key(seed), 3)
    return {
        "inverse_factor": draw_inverse_factor(jax.random.fold_in(key_list[2], 71), 0),
        "alpha_vector": bell_draw(key_list[1], (N,), 0.3, 2.0, jnp.float32),
    }


def reference(inverse_factor, alpha_vector):
    gram = jnp.dot(inverse_factor.T, inverse_factor, preferred_element_type=jnp.float32)
    return gram - alpha_vector[:, None] * alpha_vector[None, :]
```

```python
import functools

import jax
import jax.numpy as jnp
from jax import lax
from jax.experimental import pallas as pl
from jax.experimental.pallas import tpu as pltpu
from jax.sharding import PartitionSpec as P

LANES = 128
MESH = pl.DeviceIdType.MESH
OFFSET = 2.0**-10


def contract(left, right):
    return lax.dot_general(
        left, right, (((0,), (0,)), ((), ())), preferred_element_type=jnp.float32
    )


def square_side(count):
    return max(side for side in range(1, count + 1) if count % side == 0 and side * side <= count)


def code_scale(order):
    scale = 1.0
    while 4 * order * scale > 2**15:
        scale /= 2
    return scale


def encode(value, scale):
    base = jnp.abs(value) * scale + OFFSET
    base = base * base
    base = base * base
    base = base * base - OFFSET**8
    return jnp.where(value < 0, -base, base).astype(jnp.bfloat16)


def decode(code, scale):
    code = code.astype(jnp.float32)
    root = jnp.sqrt(jnp.sqrt(jnp.sqrt(jnp.abs(code) + OFFSET**8)))
    root = (root - OFFSET) * (1.0 / scale)
    return jnp.where(code < 0, -root, root)


def gram_kernel(n, scale, x_ref, out_ref, cols, rows, acc, coded, sems):
    (x_send, z_recv, right_send, left_send, r_recv, r_send, d_send, o_recv, o_send) = sems
    s = lax.axis_index("row")
    c = lax.axis_index("col")
    z, h = lax.div(c, 2), lax.rem(c, 2)
    parts = n // 2
    g = x_ref.shape[0] // n
    w = g // n
    steps = n * n
    side = n // square_side(n), square_side(n)
    s_hi, s_lo = lax.div(s, side[1]), lax.rem(s, side[1])
    row_core, row_part = lax.div(z, parts), lax.rem(z, parts)
    on_row_core = h == row_core
    lo_peers = [s_hi * side[1] + lax.rem(s_lo + i, side[1]) for i in range(1, side[1])]
    hi_peers = [lax.rem(s_hi + i, side[0]) * side[1] + s_lo for i in range(1, side[0])]

    def slot(f, b):
        k, j = lax.div(f, n), lax.rem(f, n)
        return (lax.div(k * (k + 1), 2) + b) * n + j

    def lanes(index, width):
        return pl.ds(pl.multiple_of(index * width, LANES), width)

    def col_group(b, p):
        return n * b + parts * h + p

    def col_piece(f, b, p):
        return cols.at[slot(f, b), :, lanes(p, w)]

    def row_piece(f, a, origin):
        return rows.at[slot(f, a), :, lanes(origin, w)]

    def remote(src, dst, send, recv, row, col):
        return pltpu.make_async_remote_copy(
            src_ref=src, dst_ref=dst, send_sem=send, recv_sem=recv,
            device_id=(row, col), device_id_type=MESH,
        )

    def scatter(act):
        for j in range(n - 1, -1, -1):
            f = n * s + j
            for p in range(parts):
                here = (s > z) | ((s == z) & (j >= parts * h + p))

                @pl.when(here)
                def _():
                    for i in range(n):
                        dest = lax.rem(s + i, n)
                        src = x_ref.at[pl.ds(j * g, g), pl.ds(pl.multiple_of(p * g + dest * w, LANES), w)]
                        sem = z_recv.at[slot(f, z), p]
                        if i == 0:
                            if act == "start":
                                pltpu.make_async_copy(src, col_piece(f, z, p), sem).start()
                        else:
                            copy = remote(src, col_piece(f, z, p), x_send.at[j, p, i - 1], sem, dest, c)
                            copy.start() if act == "start" else copy.wait_send()

    scatter("start")

    for j in range(n):
        for p in range(parts):

            @pl.when((j >= parts * h) & (j < parts * h + p))
            def _():
                @pl.loop(0, n)
                def _(k):
                    cols[slot(n * k + j, k), :, p * w:(p + 1) * w] = jnp.zeros((g, w), cols.dtype)

    @pl.loop(0, n * n)
    def _(i):
        acc[i] = jnp.zeros(acc.shape[1:], acc.dtype)

    def z_copy(f, b, p, step):
        send = right_send if step > 0 else left_send
        piece = col_piece(f, b, p)
        return remote(piece, piece, send.at[slot(f, b), p], z_recv.at[slot(f, b), p], s, c + 2 * step)

    def z_wait(f, b, p):
        piece = col_piece(f, b, p)
        pltpu.make_async_copy(piece, piece, z_recv.at[slot(f, b), p]).wait()

    def exists(f, b, p):
        return (b >= 0) & (b < n) & (col_group(b, p) <= f)

    def r_copy(f, a, origin, row, index, src=None):
        piece = row_piece(f, a, origin)
        return remote(
            piece if src is None else src, piece, r_send.at[slot(f, a), index],
            r_recv.at[slot(f, a), origin], row, c,
        )

    def d_copy(f, a, origin, src=None):
        piece = row_piece(f, a, origin)
        return remote(
            piece if src is None else src, piece, d_send.at[slot(f, a), origin],
            r_recv.at[slot(f, a), origin], s, c + 1 - 2 * h,
        )

    def r_wait(f, a, origin):
        piece = row_piece(f, a, origin)
        pltpu.make_async_copy(piece, piece, r_recv.at[slot(f, a), origin]).wait()

    def by_order(a, action):
        @pl.when(lax.rem(a, 2) == 0)
        def _():
            action(lo_peers, hi_peers)

        @pl.when(lax.rem(a, 2) == 1)
        def _():
            action(hi_peers, lo_peers)

    def own_rows(f, a, p, act):
        src = col_piece(f, a, p)
        copies = [r_copy(f, a, s, peer, i, src) for i, peer in enumerate(lo_peers + hi_peers)]
        copies.append(d_copy(f, a, s, src))
        for copy in copies:
            copy.start() if act == "start" else copy.wait_send()
        if act == "start":
            rows[slot(f, a), :, lanes(s, w)] = cols[slot(f, a), :, lanes(p, w)]

    own_count = len(lo_peers) + len(hi_peers)

    def relay_rows(f, a, act):
        def action(first, second):
            index = own_count
            for origin in first:
                if act == "start":
                    r_wait(f, a, origin)
                copies = []
                for peer in second:
                    copies.append(r_copy(f, a, origin, peer, index))
                    index += 1
                copies.append(d_copy(f, a, origin))
                for copy in copies:
                    copy.start() if act == "start" else copy.wait_send()

        by_order(a, action)

    def last_rows(f, a, act):
        def full(first, second, first_is_lo):
            for i in range(len(second)):
                origins = [second[i]]
                for m in range(len(first)):
                    if first_is_lo:
                        hi = lax.div(second[i], side[1])
                        lo = lax.rem(first[m], side[1])
                    else:
                        hi = lax.div(first[m], side[1])
                        lo = lax.rem(second[i], side[1])
                    origins.append(hi * side[1] + lo)
                for origin in origins:
                    if act == "start":
                        r_wait(f, a, origin)
                    copy = d_copy(f, a, origin)
                    copy.start() if act == "start" else copy.wait_send()

        @pl.when(lax.rem(a, 2) == 0)
        def _():
            full(lo_peers, hi_peers, True)

        @pl.when(lax.rem(a, 2) == 1)
        def _():
            full(hi_peers, lo_peers, False)

    def pass_on(f, b, p, act, wait):
        if act == "start" and wait:
            z_wait(f, b, p)

        @pl.when((b <= z) & (z < n - 1))
        def _():
            copy = z_copy(f, b, p, 1)
            copy.start() if act == "start" else copy.wait_send()

        @pl.when((b >= z) & (z > 0))
        def _():
            copy = z_copy(f, b, p, -1)
            copy.start() if act == "start" else copy.wait_send()

        @pl.when(on_row_core & (row_part == p))
        def _():
            own_rows(f, b, p, act)

    def own_columns(f, act):
        for p in range(parts):

            @pl.when(exists(f, z, p))
            def _():
                pass_on(f, z, p, act, True)

    def other_columns(f, act):
        for distance in range(1, n):
            for b in (z - distance, z + distance):
                for p in range(parts):

                    @pl.when(exists(f, b, p))
                    def _():
                        pass_on(f, b, p, act, True)

    def row_blocks(f):
        k, j = lax.div(f, n), lax.rem(f, n)
        return k + (z <= j).astype(jnp.int32)

    def col_blocks(f):
        k, j = lax.div(f, n), lax.rem(f, n)
        return k + (parts * h <= j).astype(jnp.int32)

    def each_row_block(f, action):
        @pl.when(on_row_core)
        def _():
            @pl.loop(0, row_blocks(f))
            def _(a):
                action(a)

    def compute(f):
        @pl.when(~on_row_core)
        def _():
            @pl.loop(0, row_blocks(f))
            def _(a):
                for origin in range(n):
                    r_wait(f, a, origin)

        @pl.loop(0, row_blocks(f))
        def _(a):
            @pl.loop(0, col_blocks(f))
            def _(b):
                acc[a * n + b] += contract(rows[slot(f, a)], cols[slot(f, b)])

    def result_copies(a, b, act):
        for half in range(2):
            index = (a * n + b) * 2 + half
            src = coded.at[index]
            dst = out_ref.at[pl.ds((2 * b + h) * parts, parts), :, lanes(s, w)]
            owner = 2 * z + half
            here = (a == s) & (half == h)

            @pl.when(here)
            def _():
                if act == "start":
                    pltpu.make_async_copy(src, dst, o_recv).start()

            @pl.when(~here)
            def _():
                copy = remote(src, dst, o_send.at[index], o_recv, a, owner)
                copy.start() if act == "start" else copy.wait_send()

    def result(a, b):
        for half in range(2):
            for p in range(parts):
                value = acc[a * n + b, half * (g // 2):(half + 1) * (g // 2), p * w:(p + 1) * w]
                coded[(a * n + b) * 2 + half, p] = encode(value, scale)
        result_copies(a, b, "start")

    def finish(f):
        k = lax.div(f, n)

        @pl.when(lax.rem(f, n) == 0)
        def _():
            @pl.loop(0, k + 1)
            def _(i):
                result(k, i)

            @pl.loop(0, k)
            def _(i):
                result(i, k)

    def guarded(f, action):
        @pl.when((f >= 0) & (f < steps))
        def _():
            action(f)

    ahead = 2
    for i in range(ahead):
        own_columns(steps - 1 - i, "start")

    @pl.loop(0, steps + 3)
    def _(t):
        f = steps - 1 - t
        guarded(f - ahead, lambda f: own_columns(f, "start"))
        guarded(f, lambda f: other_columns(f, "start"))
        guarded(f + 1, lambda f: each_row_block(f, lambda a: relay_rows(f, a, "start")))
        guarded(f + 2, lambda f: each_row_block(f, lambda a: last_rows(f, a, "start")))

        def last(f):
            compute(f)
            finish(f)

        guarded(f + 3, last)

    scatter("wait")

    @pl.loop(0, steps)
    def _(f):
        own_columns(f, "wait")
        other_columns(f, "wait")
        each_row_block(f, lambda a: relay_rows(f, a, "wait"))
        each_row_block(f, lambda a: last_rows(f, a, "wait"))

    @pl.loop(0, n)
    def _(a):
        @pl.loop(0, n)
        def _(b):
            result_copies(a, b, "wait")

    pltpu.make_async_copy(out_ref, out_ref, o_recv).wait()


def planes(inverse_factor, alpha_vector):
    n = lax.axis_size("row")
    n_col = lax.axis_size("col")
    tile_rows, tile_cols = inverse_factor.shape
    order = alpha_vector.shape[0]
    parts, g = n // 2, tile_rows // n
    w = g // n
    scale = code_scale(order)
    slots = n * (n + 1) // 2 * n
    sem = pltpu.SemaphoreType.DMA
    side = n // square_side(n), square_side(n)
    sends = (side[0] - 1) + (side[1] - 1) + (side[0] - 1) * (side[1] - 1)
    coded = pl.pallas_call(
        functools.partial(gram_kernel, n, scale),
        out_shape=jax.ShapeDtypeStruct((n * n, g // 2, n * w), jnp.bfloat16),
        in_specs=[pl.BlockSpec(memory_space=pl.ANY)],
        out_specs=pl.BlockSpec(memory_space=pl.ANY),
        scratch_shapes=[
            pltpu.VMEM((slots, g, parts * w), jnp.bfloat16),
            pltpu.VMEM((slots, g, g), jnp.bfloat16),
            pltpu.VMEM((n * n, g, parts * w), jnp.float32),
            pltpu.VMEM((n * n * 2, parts, g // 2, w), jnp.bfloat16),
            (
                sem((n, parts, n - 1)),
                sem((slots, parts)),
                sem((slots, parts)),
                sem((slots, parts)),
                sem((slots, n)),
                sem((slots, sends)),
                sem((slots, n)),
                sem,
                sem((n * n * 2,)),
            ),
        ],
        compiler_params=pltpu.CompilerParams(
            has_side_effects=True, vmem_limit_bytes=60 * 2**20
        ),
    )(inverse_factor)
    first_row = (lax.axis_index("row") * n_col + lax.axis_index("col")) * (order // (n * n_col))
    own_alpha = lax.dynamic_slice_in_dim(alpha_vector, first_row, order // (n * n_col), 0)
    gram = decode(coded, scale).transpose(1, 0, 2).reshape(g // 2, order)
    return gram - own_alpha[:, None] * alpha_vector[None, :]


def layers(inverse_factor, alpha_vector):
    layer = lax.axis_index("row")
    column = lax.axis_index("col")
    n_row = lax.axis_size("row")
    n_col = lax.axis_size("col")
    tile_rows, tile_cols = inverse_factor.shape
    ratio = n_col // n_row
    width = tile_cols // n_row
    gathered = lax.all_gather(inverse_factor, "col", axis=0, tiled=False)
    block_in_layer = column * width // tile_cols
    first_col = column * width % tile_cols

    def owned_by(dest):
        start = (dest * ratio + block_in_layer, 0, first_col)
        return lax.dynamic_slice(gathered, start, (1, tile_rows, width))[0]

    sides = (n_row // square_side(n_row), square_side(n_row))
    place = (layer // sides[1], layer % sides[1])

    def index(first, second, order):
        return second * sides[1] + first if order else first * sides[1] + second

    def reduced(block, order):
        chunk = block // ratio
        n_first, n_second = (sides[1], sides[0]) if order else sides
        first, second = (place[1], place[0]) if order else place

        def dest(u, v, s, t):
            return index((u - s) % n_first, (v - t) % n_second, order)

        def partial_of(s, t):
            left = owned_by(dest(first, second, s, t))
            return contract(left, gathered[block])

        def owes(u, v, s, t):
            g = index(u, v, order)
            return g >= chunk and g >= dest(u, v, s, t)

        places = [(u, v) for u in range(n_first) for v in range(n_second)]

        def first_hop(s, t):
            pairs = [
                (index(u, v, order), dest(u, v, s, 0)) for u, v in places if owes(u, v, s, t)
            ]
            if not pairs:
                return None
            return lax.ppermute(partial_of(s, t).astype(jnp.float16), "row", pairs)

        def second_hop(value, t):
            pairs = []
            for u, v in places:
                if any(owes((u + s) % n_first, v, s, t) for s in range(n_first)):
                    pairs.append((index(u, v, order), dest(u, v, 0, t)))
            if not pairs:
                return None
            return lax.ppermute(value.astype(jnp.float16), "row", pairs)

        def add(total, part):
            return total if part is None else total + part.astype(jnp.float32)

        hops = {}
        for t in range(n_second - 1, -1, -1):
            for s in range(n_first - 1, 0, -1):
                hops[s, t] = first_hop(s, t)

        def finish():
            parts = []
            for t in range(n_second - 1, 0, -1):
                value = partial_of(0, t)
                for s in range(1, n_first):
                    value = add(value, hops[s, t])
                parts.append(second_hop(value, t))
            total = partial_of(0, 0)
            for s in range(1, n_first):
                total = add(total, hops[s, 0])
            for part in parts:
                total = add(total, part)
            return total

        return finish

    first_row = (layer * n_col + column) * width
    own_alpha = lax.dynamic_slice_in_dim(alpha_vector, first_row, width, 0)
    pieces = []
    for finish in [reduced(block, block % 2) for block in range(n_col)]:
        alpha = lax.slice_in_dim(
            alpha_vector, len(pieces) * tile_cols, (len(pieces) + 1) * tile_cols
        )
        pieces.append(finish() - own_alpha[:, None] * alpha[None, :])
    return jnp.concatenate(pieces, axis=1)


def per_device(inverse_factor, alpha_vector):
    n_row, n_col = lax.axis_size("row"), lax.axis_size("col")
    aligned = inverse_factor.shape[0] % (n_row * n_row * LANES) == 0
    if n_col == 2 * n_row and n_row % 2 == 0 and aligned:
        return planes(inverse_factor, alpha_vector)
    return layers(inverse_factor, alpha_vector)


def solution(mesh):
    in_specs = (P("row", "col"), P())
    out_specs = P(("row", "col"), None)
    return jax.shard_map(
        per_device, mesh=mesh, in_specs=in_specs, out_specs=out_specs, check_vma=False
    )
```

```python
import functools

import jax
import jax.numpy as jnp
from jax import lax
from jax.experimental import pallas as pl
from jax.experimental.pallas import tpu as pltpu
from jax.sharding import PartitionSpec as P

LANES = 128
MESH = pl.DeviceIdType.MESH
OFFSET = 2.0**-10
SCATTER_AHEAD = 16
OWN_AHEAD = 2
SKEW = (3, 6, 8)


def contract(left, right):
    return lax.dot_general(
        left, right, (((0,), (0,)), ((), ())), preferred_element_type=jnp.float32
    )


def square_side(count):
    return max(side for side in range(1, count + 1) if count % side == 0 and side * side <= count)


def code_scale(order):
    scale = 1.0
    while 4 * order * scale > 2**15:
        scale /= 2
    return scale


def encode(value, scale):
    base = jnp.abs(value) * scale + OFFSET
    base = base * base
    base = base * base
    base = base * base - OFFSET**8
    return jnp.where(value < 0, -base, base).astype(jnp.bfloat16)


def decode(code, scale):
    code = code.astype(jnp.float32)
    power = jnp.abs(code) + OFFSET**8
    fourth = lax.rsqrt(lax.rsqrt(power))
    root = fourth * lax.rsqrt(fourth) - OFFSET
    return jnp.where(code < 0, -root, root) * (1.0 / scale)


def output_kernel(scale, code_ref, own_ref, alpha_ref, out_ref):
    width = code_ref.shape[2]
    for i in range(code_ref.shape[0]):
        at = slice(i * width, (i + 1) * width)
        out_ref[:, at] = decode(code_ref[i], scale) - own_ref[...] * alpha_ref[:, at]


def gram_kernel(n, scale, x_ref, out_ref, cols, rows, acc, coded, sems):
    (x_send, z_recv, right_send, left_send, r_recv, r_send, d_send, o_recv, o_send) = sems
    s = lax.axis_index("row")
    c = lax.axis_index("col")
    z, h = lax.div(c, 2), lax.rem(c, 2)
    parts = n // 2
    g = x_ref.shape[0] // n
    w = g // n
    steps = n * n
    side = n // square_side(n), square_side(n)
    s_hi, s_lo = lax.div(s, side[1]), lax.rem(s, side[1])
    row_core, row_part = lax.div(z, parts), lax.rem(z, parts)
    on_row_core = h == row_core
    lo_peers = [s_hi * side[1] + lax.rem(s_lo + i, side[1]) for i in range(1, side[1])]
    hi_peers = [lax.rem(s_hi + i, side[0]) * side[1] + s_lo for i in range(1, side[0])]

    def slot(f, b):
        k, j = lax.div(f, n), lax.rem(f, n)
        return (lax.div(k * (k + 1), 2) + b) * n + j

    def lanes(index, width):
        return pl.ds(pl.multiple_of(index * width, LANES), width)

    def col_group(b, p):
        return n * b + parts * h + p

    def exists(f, b, p):
        return (b >= 0) & (b < n) & (col_group(b, p) <= f)

    def col_piece(f, b, p):
        return cols.at[f, :, lanes(b * parts + p, w)]

    def row_piece(f, a, origin):
        return rows.at[slot(f, a), :, lanes(origin, w)]

    def remote(src, dst, send, recv, row, col):
        return pltpu.make_async_remote_copy(
            src_ref=src, dst_ref=dst, send_sem=send, recv_sem=recv,
            device_id=(row, col), device_id_type=MESH,
        )

    def scatter(f, act):
        j = lax.rem(f, n)
        for p in range(parts):

            @pl.when((lax.div(f, n) == s) & exists(f, z, p))
            def _():
                for i in range(n):
                    dest = lax.rem(s + i, n)
                    src = x_ref.at[
                        pl.ds(pl.multiple_of(j * g, g), g),
                        pl.ds(pl.multiple_of(p * g + dest * w, LANES), w),
                    ]
                    sem = z_recv.at[slot(f, z), p]
                    if i > 0:
                        copy = remote(src, col_piece(f, z, p), x_send.at[j, p, i - 1], sem, dest, c)
                        copy.start() if act == "start" else copy.wait_send()
                    elif act == "start":
                        pltpu.make_async_copy(src, col_piece(f, z, p), sem).start()

    def z_copy(f, b, p, step):
        send = right_send if step > 0 else left_send
        piece = col_piece(f, b, p)
        return remote(piece, piece, send.at[slot(f, b), p], z_recv.at[slot(f, b), p], s, c + 2 * step)

    def z_wait(f, b, p):
        piece = col_piece(f, b, p)
        pltpu.make_async_copy(piece, piece, z_recv.at[slot(f, b), p]).wait()

    def r_copy(f, a, origin, row, index, src=None):
        piece = row_piece(f, a, origin)
        return remote(
            piece if src is None else src, piece, r_send.at[slot(f, a), index],
            r_recv.at[slot(f, a), origin], row, c,
        )

    def d_copy(f, a, origin, src=None):
        piece = row_piece(f, a, origin)
        return remote(
            piece if src is None else src, piece, d_send.at[slot(f, a), origin],
            r_recv.at[slot(f, a), origin], s, c + 1 - 2 * h,
        )

    def r_wait(f, a, origin):
        piece = row_piece(f, a, origin)
        pltpu.make_async_copy(piece, piece, r_recv.at[slot(f, a), origin]).wait()

    def by_order(a, action):
        @pl.when(lax.rem(a, 2) == 0)
        def _():
            action(lo_peers, hi_peers)

        @pl.when(lax.rem(a, 2) == 1)
        def _():
            action(hi_peers, lo_peers)

    def own_rows(f, a, p, act):
        src = col_piece(f, a, p)
        copies = [r_copy(f, a, s, peer, i, src) for i, peer in enumerate(lo_peers + hi_peers)]
        copies.append(d_copy(f, a, s, src))
        for copy in copies:
            copy.start() if act == "start" else copy.wait_send()
        if act == "start":
            rows[slot(f, a), :, lanes(s, w)] = cols[f, :, lanes(a * parts + p, w)]

    own_count = len(lo_peers) + len(hi_peers)

    def relay_rows(f, a, act):
        def action(first, second):
            index = own_count
            for origin in first:
                if act == "start":
                    r_wait(f, a, origin)
                copies = []
                for peer in second:
                    copies.append(r_copy(f, a, origin, peer, index))
                    index += 1
                copies.append(d_copy(f, a, origin))
                for copy in copies:
                    copy.start() if act == "start" else copy.wait_send()

        by_order(a, action)

    def last_rows(f, a, act):
        def full(first, second, first_is_lo):
            for i in range(len(second)):
                origins = [second[i]]
                for m in range(len(first)):
                    if first_is_lo:
                        hi = lax.div(second[i], side[1])
                        lo = lax.rem(first[m], side[1])
                    else:
                        hi = lax.div(first[m], side[1])
                        lo = lax.rem(second[i], side[1])
                    origins.append(hi * side[1] + lo)
                for origin in origins:
                    if act == "start":
                        r_wait(f, a, origin)
                    copy = d_copy(f, a, origin)
                    copy.start() if act == "start" else copy.wait_send()

        @pl.when(lax.rem(a, 2) == 0)
        def _():
            full(lo_peers, hi_peers, True)

        @pl.when(lax.rem(a, 2) == 1)
        def _():
            full(hi_peers, lo_peers, False)

    def pass_on(f, b, p, act, wait):
        if act == "start" and wait:
            z_wait(f, b, p)

        @pl.when((b <= z) & (z < n - 1))
        def _():
            copy = z_copy(f, b, p, 1)
            copy.start() if act == "start" else copy.wait_send()

        @pl.when((b >= z) & (z > 0))
        def _():
            copy = z_copy(f, b, p, -1)
            copy.start() if act == "start" else copy.wait_send()

        @pl.when(on_row_core & (row_part == p))
        def _():
            own_rows(f, b, p, act)

    def own_columns(f, act):
        for p in range(parts):

            @pl.when(exists(f, z, p))
            def _():
                pass_on(f, z, p, act, True)

    def other_columns(f, act):
        for distance in range(1, n):
            for b in (z - distance, z + distance):
                for p in range(parts):

                    @pl.when(exists(f, b, p))
                    def _():
                        pass_on(f, b, p, act, True)

    def row_blocks(f):
        k, j = lax.div(f, n), lax.rem(f, n)
        return k + (z <= j).astype(jnp.int32)

    def col_blocks(f):
        k, j = lax.div(f, n), lax.rem(f, n)
        return k + (parts * h <= j).astype(jnp.int32)

    def each_row_block(f, action):
        @pl.when(on_row_core)
        def _():
            @pl.loop(0, row_blocks(f))
            def _(a):
                action(a)

    def compute(f):
        @pl.when(~on_row_core)
        def _():
            @pl.loop(0, row_blocks(f))
            def _(a):
                for origin in range(n):
                    r_wait(f, a, origin)

        @pl.loop(0, row_blocks(f))
        def _(a):
            for blocks in range(1, n + 1):

                @pl.when(col_blocks(f) == blocks)
                def _():
                    width = blocks * parts * w
                    acc[a, :, :width] += contract(rows[slot(f, a)], cols[f, :, :width])

    def result_copies(a, b, act):
        for half in range(2):
            index = (a * n + b) * 2 + half
            src = coded.at[index]
            dst = out_ref.at[pl.ds((2 * b + h) * parts, parts), :, lanes(s, w)]
            owner = 2 * z + half
            here = (a == s) & (half == h)

            @pl.when(here)
            def _():
                if act == "start":
                    pltpu.make_async_copy(src, dst, o_recv).start()

            @pl.when(~here)
            def _():
                copy = remote(src, dst, o_send.at[index], o_recv, a, owner)
                copy.start() if act == "start" else copy.wait_send()

    def result(a, b):
        for half in range(2):
            for p in range(parts):
                value = acc[a, half * (g // 2):(half + 1) * (g // 2), lanes(b * parts + p, w)]
                coded[(a * n + b) * 2 + half, p] = encode(value, scale)
        result_copies(a, b, "start")

    def finish(f):
        k = lax.div(f, n)

        @pl.when(lax.rem(f, n) == 0)
        def _():
            @pl.loop(0, k + 1)
            def _(i):
                result(k, i)

            @pl.loop(0, k)
            def _(i):
                result(i, k)

    def guarded(f, action):
        @pl.when((f >= 0) & (f < steps))
        def _():
            action(f)

    for i in range(SCATTER_AHEAD):
        scatter(jnp.int32(steps - 1 - i), "start")

    for j in range(n):
        for p in range(parts):

            @pl.when((j >= parts * h) & (j < parts * h + p))
            def _():
                @pl.loop(0, n)
                def _(k):
                    cols[n * k + j, :, lanes(k * parts + p, w)] = jnp.zeros((g, w), cols.dtype)

    @pl.loop(0, n)
    def _(i):
        acc[i] = jnp.zeros(acc.shape[1:], acc.dtype)

    for i in range(OWN_AHEAD):
        own_columns(jnp.int32(steps - 1 - i), "start")

    @pl.loop(0, steps + SKEW[2])
    def _(t):
        f = steps - 1 - t
        guarded(f - SCATTER_AHEAD, lambda f: scatter(f, "start"))
        guarded(f - OWN_AHEAD, lambda f: own_columns(f, "start"))
        guarded(f, lambda f: other_columns(f, "start"))
        guarded(f + SKEW[0], lambda f: each_row_block(f, lambda a: relay_rows(f, a, "start")))
        guarded(f + SKEW[1], lambda f: each_row_block(f, lambda a: last_rows(f, a, "start")))

        def last(f):
            compute(f)
            finish(f)

        guarded(f + SKEW[2], last)

    @pl.loop(0, steps)
    def _(f):
        scatter(f, "wait")
        own_columns(f, "wait")
        other_columns(f, "wait")
        each_row_block(f, lambda a: relay_rows(f, a, "wait"))
        each_row_block(f, lambda a: last_rows(f, a, "wait"))

    @pl.loop(0, n)
    def _(a):
        @pl.loop(0, n)
        def _(b):
            result_copies(a, b, "wait")

    pltpu.make_async_copy(out_ref, out_ref, o_recv).wait()


def planes(inverse_factor, alpha_vector):
    n = lax.axis_size("row")
    n_col = lax.axis_size("col")
    tile_rows, tile_cols = inverse_factor.shape
    order = alpha_vector.shape[0]
    parts, g = n // 2, tile_rows // n
    w = g // n
    scale = code_scale(order)
    slots = n * (n + 1) // 2 * n
    sem = pltpu.SemaphoreType.DMA
    side = n // square_side(n), square_side(n)
    sends = (side[0] - 1) + (side[1] - 1) + (side[0] - 1) * (side[1] - 1)
    coded = pl.pallas_call(
        functools.partial(gram_kernel, n, scale),
        out_shape=jax.ShapeDtypeStruct((n * n, g // 2, n * w), jnp.bfloat16),
        in_specs=[pl.BlockSpec(memory_space=pl.ANY)],
        out_specs=pl.BlockSpec(memory_space=pl.ANY),
        scratch_shapes=[
            pltpu.VMEM((n * n, g, n * parts * w), jnp.bfloat16),
            pltpu.VMEM((slots, g, g), jnp.bfloat16),
            pltpu.VMEM((n, g, n * parts * w), jnp.float32),
            pltpu.VMEM((n * n * 2, parts, g // 2, w), jnp.bfloat16),
            (
                sem((n, parts, n - 1)),
                sem((slots, parts)),
                sem((slots, parts)),
                sem((slots, parts)),
                sem((slots, n)),
                sem((slots, sends)),
                sem((slots, n)),
                sem,
                sem((n * n * 2,)),
            ),
        ],
        compiler_params=pltpu.CompilerParams(
            has_side_effects=True, vmem_limit_bytes=60 * 2**20
        ),
    )(inverse_factor)
    first_row = (lax.axis_index("row") * n_col + lax.axis_index("col")) * (order // (n * n_col))
    own_alpha = lax.dynamic_slice_in_dim(alpha_vector, first_row, order // (n * n_col), 0)
    return pl.pallas_call(
        functools.partial(output_kernel, scale),
        out_shape=jax.ShapeDtypeStruct((g // 2, order), jnp.float32),
        grid=(n,),
        in_specs=[
            pl.BlockSpec((n, g // 2, g), lambda i: (i, 0, 0)),
            pl.BlockSpec((g // 2, 1), lambda i: (0, 0)),
            pl.BlockSpec((1, n * g), lambda i: (0, i)),
        ],
        out_specs=pl.BlockSpec((g // 2, n * g), lambda i: (0, i)),
    )(coded, own_alpha[:, None], alpha_vector[None, :])


def layers(inverse_factor, alpha_vector):
    layer = lax.axis_index("row")
    column = lax.axis_index("col")
    n_row = lax.axis_size("row")
    n_col = lax.axis_size("col")
    tile_rows, tile_cols = inverse_factor.shape
    ratio = n_col // n_row
    width = tile_cols // n_row
    gathered = lax.all_gather(inverse_factor, "col", axis=0, tiled=False)
    block_in_layer = column * width // tile_cols
    first_col = column * width % tile_cols

    def owned_by(dest):
        start = (dest * ratio + block_in_layer, 0, first_col)
        return lax.dynamic_slice(gathered, start, (1, tile_rows, width))[0]

    sides = (n_row // square_side(n_row), square_side(n_row))
    place = (layer // sides[1], layer % sides[1])

    def index(first, second, order):
        return second * sides[1] + first if order else first * sides[1] + second

    def reduced(block, order):
        chunk = block // ratio
        n_first, n_second = (sides[1], sides[0]) if order else sides
        first, second = (place[1], place[0]) if order else place

        def dest(u, v, s, t):
            return index((u - s) % n_first, (v - t) % n_second, order)

        def partial_of(s, t):
            left = owned_by(dest(first, second, s, t))
            return contract(left, gathered[block])

        def owes(u, v, s, t):
            g = index(u, v, order)
            return g >= chunk and g >= dest(u, v, s, t)

        places = [(u, v) for u in range(n_first) for v in range(n_second)]

        def first_hop(s, t):
            pairs = [
                (index(u, v, order), dest(u, v, s, 0)) for u, v in places if owes(u, v, s, t)
            ]
            if not pairs:
                return None
            return lax.ppermute(partial_of(s, t).astype(jnp.float16), "row", pairs)

        def second_hop(value, t):
            pairs = []
            for u, v in places:
                if any(owes((u + s) % n_first, v, s, t) for s in range(n_first)):
                    pairs.append((index(u, v, order), dest(u, v, 0, t)))
            if not pairs:
                return None
            return lax.ppermute(value.astype(jnp.float16), "row", pairs)

        def add(total, part):
            return total if part is None else total + part.astype(jnp.float32)

        hops = {}
        for t in range(n_second - 1, -1, -1):
            for s in range(n_first - 1, 0, -1):
                hops[s, t] = first_hop(s, t)

        def finish():
            parts = []
            for t in range(n_second - 1, 0, -1):
                value = partial_of(0, t)
                for s in range(1, n_first):
                    value = add(value, hops[s, t])
                parts.append(second_hop(value, t))
            total = partial_of(0, 0)
            for s in range(1, n_first):
                total = add(total, hops[s, 0])
            for part in parts:
                total = add(total, part)
            return total

        return finish

    first_row = (layer * n_col + column) * width
    own_alpha = lax.dynamic_slice_in_dim(alpha_vector, first_row, width, 0)
    pieces = []
    for finish in [reduced(block, block % 2) for block in range(n_col)]:
        alpha = lax.slice_in_dim(
            alpha_vector, len(pieces) * tile_cols, (len(pieces) + 1) * tile_cols
        )
        pieces.append(finish() - own_alpha[:, None] * alpha[None, :])
    return jnp.concatenate(pieces, axis=1)


def per_device(inverse_factor, alpha_vector):
    n_row, n_col = lax.axis_size("row"), lax.axis_size("col")
    aligned = inverse_factor.shape[0] % (n_row * n_row * LANES) == 0
    if n_col == 2 * n_row and n_row % 2 == 0 and aligned:
        return planes(inverse_factor, alpha_vector)
    return layers(inverse_factor, alpha_vector)


def solution(mesh):
    in_specs = (P("row", "col"), P())
    out_specs = P(("row", "col"), None)
    return jax.shard_map(
        per_device, mesh=mesh, in_specs=in_specs, out_specs=out_specs, check_vma=False
    )
```

```python
import functools

import jax
import jax.numpy as jnp
from jax import lax
from jax.experimental import pallas as pl
from jax.experimental.pallas import tpu as pltpu
from jax.sharding import PartitionSpec as P

LANES = 128
MESH = pl.DeviceIdType.MESH
OFFSET = 2.0**-10
SCATTER_AHEAD = 16
OWN_AHEAD = 1
SKEW = (2, 5, 7)
EDGE_SKEW = (1, 3, 5)


def contract(left, right):
    return lax.dot_general(
        left, right, (((0,), (0,)), ((), ())), preferred_element_type=jnp.float32
    )


def square_side(count):
    return max(side for side in range(1, count + 1) if count % side == 0 and side * side <= count)


def code_scale(order):
    scale = 1.0
    while 4 * order * scale > 2**15:
        scale /= 2
    return scale


def encode(value, scale):
    base = jnp.abs(value) * scale + OFFSET
    base = base * base
    base = base * base
    base = base * base - OFFSET**8
    return jnp.where(value < 0, -base, base).astype(jnp.bfloat16)


def decode(code, scale):
    code = code.astype(jnp.float32)
    power = jnp.abs(code) + OFFSET**8
    fourth = lax.rsqrt(lax.rsqrt(power))
    root = fourth * lax.rsqrt(fourth) - OFFSET
    return jnp.where(code < 0, -root, root) * (1.0 / scale)


def output_kernel(scale, code_ref, own_ref, alpha_ref, out_ref):
    width = code_ref.shape[2]
    for i in range(code_ref.shape[0]):
        at = slice(i * width, (i + 1) * width)
        out_ref[:, at] = decode(code_ref[i], scale) - own_ref[...] * alpha_ref[:, at]


def gram_kernel(n, scale, x_ref, out_ref, cols, rows, acc, coded, sems):
    (x_send, z_recv, right_send, left_send, r_recv, r_send, d_send, o_recv, o_send) = sems
    s = lax.axis_index("row")
    c = lax.axis_index("col")
    z, h = lax.div(c, 2), lax.rem(c, 2)
    parts = n // 2
    g = x_ref.shape[0] // n
    w = g // n
    steps = n * n
    side = n // square_side(n), square_side(n)
    s_hi, s_lo = lax.div(s, side[1]), lax.rem(s, side[1])
    row_core, row_part = lax.div(z, parts), lax.rem(z, parts)
    on_row_core = h == row_core
    lo_peers = [s_hi * side[1] + lax.rem(s_lo + i, side[1]) for i in range(1, side[1])]
    hi_peers = [lax.rem(s_hi + i, side[0]) * side[1] + s_lo for i in range(1, side[0])]

    def slot(f, b):
        k, j = lax.div(f, n), lax.rem(f, n)
        return (lax.div(k * (k + 1), 2) + b) * n + j

    def lanes(index, width):
        return pl.ds(pl.multiple_of(index * width, LANES), width)

    def col_group(b, p):
        return n * b + parts * h + p

    def exists(f, b, p):
        return (b >= 0) & (b < n) & (col_group(b, p) <= f)

    def col_piece(f, b, p):
        return cols.at[f, :, lanes(b * parts + p, w)]

    def row_piece(f, a, origin):
        return rows.at[slot(f, a), :, lanes(origin, w)]

    def remote(src, dst, send, recv, row, col):
        return pltpu.make_async_remote_copy(
            src_ref=src, dst_ref=dst, send_sem=send, recv_sem=recv,
            device_id=(row, col), device_id_type=MESH,
        )

    def scatter(f, act):
        j = lax.rem(f, n)
        for p in range(parts):

            @pl.when((lax.div(f, n) == s) & exists(f, z, p))
            def _():
                for i in range(n):
                    dest = lax.rem(s + i, n)
                    src = x_ref.at[
                        pl.ds(pl.multiple_of(j * g, g), g),
                        pl.ds(pl.multiple_of(p * g + dest * w, LANES), w),
                    ]
                    sem = z_recv.at[slot(f, z), p]
                    if i > 0:
                        copy = remote(src, col_piece(f, z, p), x_send.at[j, p, i - 1], sem, dest, c)
                        copy.start() if act == "start" else copy.wait_send()
                    elif act == "start":
                        pltpu.make_async_copy(src, col_piece(f, z, p), sem).start()

    def z_copy(f, b, p, step):
        send = right_send if step > 0 else left_send
        piece = col_piece(f, b, p)
        return remote(piece, piece, send.at[slot(f, b), p], z_recv.at[slot(f, b), p], s, c + 2 * step)

    def z_wait(f, b, p):
        piece = col_piece(f, b, p)
        pltpu.make_async_copy(piece, piece, z_recv.at[slot(f, b), p]).wait()

    def r_copy(f, a, origin, row, index, src=None):
        piece = row_piece(f, a, origin)
        return remote(
            piece if src is None else src, piece, r_send.at[slot(f, a), index],
            r_recv.at[slot(f, a), origin], row, c,
        )

    def d_copy(f, a, origin, src=None):
        piece = row_piece(f, a, origin)
        return remote(
            piece if src is None else src, piece, d_send.at[slot(f, a), origin],
            r_recv.at[slot(f, a), origin], s, c + 1 - 2 * h,
        )

    def r_wait(f, a, origin):
        piece = row_piece(f, a, origin)
        pltpu.make_async_copy(piece, piece, r_recv.at[slot(f, a), origin]).wait()

    def by_order(turn, action):
        @pl.when(lax.rem(turn, 2) == 0)
        def _():
            action(lo_peers, hi_peers)

        @pl.when(lax.rem(turn, 2) == 1)
        def _():
            action(hi_peers, lo_peers)

    def own_rows(f, a, p, act):
        src = col_piece(f, a, p)
        copies = [r_copy(f, a, s, peer, i, src) for i, peer in enumerate(lo_peers + hi_peers)]
        copies.append(d_copy(f, a, s, src))
        for copy in copies:
            copy.start() if act == "start" else copy.wait_send()
        if act == "start":
            rows[slot(f, a), :, lanes(s, w)] = cols[f, :, lanes(a * parts + p, w)]

    own_count = len(lo_peers) + len(hi_peers)

    def relay_rows(f, a, act):
        def action(first, second):
            index = own_count
            for origin in first:
                if act == "start":
                    r_wait(f, a, origin)
                copies = []
                for peer in second:
                    copies.append(r_copy(f, a, origin, peer, index))
                    index += 1
                copies.append(d_copy(f, a, origin))
                for copy in copies:
                    copy.start() if act == "start" else copy.wait_send()

        by_order(f + a, action)

    def last_rows(f, a, act):
        def full(first, second, first_is_lo):
            for i in range(len(second)):
                origins = [second[i]]
                for m in range(len(first)):
                    if first_is_lo:
                        hi = lax.div(second[i], side[1])
                        lo = lax.rem(first[m], side[1])
                    else:
                        hi = lax.div(first[m], side[1])
                        lo = lax.rem(second[i], side[1])
                    origins.append(hi * side[1] + lo)
                for origin in origins:
                    if act == "start":
                        r_wait(f, a, origin)
                    copy = d_copy(f, a, origin)
                    copy.start() if act == "start" else copy.wait_send()

        @pl.when(lax.rem(f + a, 2) == 0)
        def _():
            full(lo_peers, hi_peers, True)

        @pl.when(lax.rem(f + a, 2) == 1)
        def _():
            full(hi_peers, lo_peers, False)

    def pass_on(f, b, p, act, wait):
        if act == "start" and wait:
            z_wait(f, b, p)

        @pl.when((b <= z) & (z < n - 1))
        def _():
            copy = z_copy(f, b, p, 1)
            copy.start() if act == "start" else copy.wait_send()

        @pl.when((b >= z) & (z > 0))
        def _():
            copy = z_copy(f, b, p, -1)
            copy.start() if act == "start" else copy.wait_send()

        @pl.when(on_row_core & (row_part == p))
        def _():
            own_rows(f, b, p, act)

    def own_columns(f, act):
        for p in range(parts):

            @pl.when(exists(f, z, p))
            def _():
                pass_on(f, z, p, act, True)

    def other_columns(f, act):
        for distance in range(1, n):
            for b in (z - distance, z + distance):
                for p in range(parts):

                    @pl.when(exists(f, b, p))
                    def _():
                        pass_on(f, b, p, act, True)

    def row_blocks(f):
        k, j = lax.div(f, n), lax.rem(f, n)
        return k + (z <= j).astype(jnp.int32)

    def col_blocks(f):
        k, j = lax.div(f, n), lax.rem(f, n)
        return k + (parts * h <= j).astype(jnp.int32)

    def each_row_block(f, action):
        @pl.when(on_row_core)
        def _():
            @pl.loop(0, row_blocks(f))
            def _(a):
                action(a)

    def compute(f):
        @pl.when(~on_row_core)
        def _():
            @pl.loop(0, row_blocks(f))
            def _(a):
                for origin in range(n):
                    r_wait(f, a, origin)

        @pl.loop(0, row_blocks(f))
        def _(a):
            for blocks in range(1, n + 1):

                @pl.when(col_blocks(f) == blocks)
                def _():
                    width = blocks * parts * w
                    acc[a, :, :width] += contract(rows[slot(f, a)], cols[f, :, :width])

    def result_copies(a, b, act):
        for half in range(2):
            index = (a * n + b) * 2 + half
            src = coded.at[index]
            dst = out_ref.at[pl.ds((2 * b + h) * parts, parts), :, lanes(s, w)]
            owner = 2 * z + half
            here = (a == s) & (half == h)

            @pl.when(here)
            def _():
                if act == "start":
                    pltpu.make_async_copy(src, dst, o_recv).start()

            @pl.when(~here)
            def _():
                copy = remote(src, dst, o_send.at[index], o_recv, a, owner)
                copy.start() if act == "start" else copy.wait_send()

    def result(a, b):
        for half in range(2):
            for p in range(parts):
                value = acc[a, half * (g // 2):(half + 1) * (g // 2), lanes(b * parts + p, w)]
                coded[(a * n + b) * 2 + half, p] = encode(value, scale)
        result_copies(a, b, "start")

    def finish(f):
        k = lax.div(f, n)

        @pl.when(lax.rem(f, n) == 0)
        def _():
            @pl.loop(0, k + 1)
            def _(i):
                result(k, i)

            @pl.loop(0, k)
            def _(i):
                result(i, k)

    def guarded(f, action):
        @pl.when((f >= 0) & (f < steps))
        def _():
            action(f)

    for i in range(SCATTER_AHEAD):
        scatter(jnp.int32(steps - 1 - i), "start")

    for j in range(n):
        for p in range(parts):

            @pl.when((j >= parts * h) & (j < parts * h + p))
            def _():
                @pl.loop(0, n)
                def _(k):
                    cols[n * k + j, :, lanes(k * parts + p, w)] = jnp.zeros((g, w), cols.dtype)

    @pl.loop(0, n)
    def _(i):
        acc[i] = jnp.zeros(acc.shape[1:], acc.dtype)

    for i in range(OWN_AHEAD):
        own_columns(jnp.int32(steps - 1 - i), "start")

    behind = [jnp.where(z == n - 1, edge, inner) for edge, inner in zip(EDGE_SKEW, SKEW)]

    @pl.loop(0, steps + SKEW[2])
    def _(t):
        f = steps - 1 - t
        guarded(f - SCATTER_AHEAD, lambda f: scatter(f, "start"))

        @pl.when(z == 0)
        def _():
            guarded(f - OWN_AHEAD, lambda f: own_columns(f, "start"))

        guarded(f, lambda f: other_columns(f, "start"))

        @pl.when(~(z == 0))
        def _():
            guarded(f - OWN_AHEAD, lambda f: own_columns(f, "start"))

        guarded(f + behind[0], lambda f: each_row_block(f, lambda a: relay_rows(f, a, "start")))
        guarded(f + behind[1], lambda f: each_row_block(f, lambda a: last_rows(f, a, "start")))

        def last(f):
            compute(f)
            finish(f)

        guarded(f + behind[2], last)

    @pl.loop(0, steps)
    def _(f):
        scatter(f, "wait")
        own_columns(f, "wait")
        other_columns(f, "wait")
        each_row_block(f, lambda a: relay_rows(f, a, "wait"))
        each_row_block(f, lambda a: last_rows(f, a, "wait"))

    @pl.loop(0, n)
    def _(a):
        @pl.loop(0, n)
        def _(b):
            result_copies(a, b, "wait")

    pltpu.make_async_copy(out_ref, out_ref, o_recv).wait()


def planes(inverse_factor, alpha_vector):
    n = lax.axis_size("row")
    n_col = lax.axis_size("col")
    tile_rows, tile_cols = inverse_factor.shape
    order = alpha_vector.shape[0]
    parts, g = n // 2, tile_rows // n
    w = g // n
    scale = code_scale(order)
    slots = n * (n + 1) // 2 * n
    sem = pltpu.SemaphoreType.DMA
    side = n // square_side(n), square_side(n)
    sends = (side[0] - 1) + (side[1] - 1) + (side[0] - 1) * (side[1] - 1)
    coded = pl.pallas_call(
        functools.partial(gram_kernel, n, scale),
        out_shape=jax.ShapeDtypeStruct((n * n, g // 2, n * w), jnp.bfloat16),
        in_specs=[pl.BlockSpec(memory_space=pl.ANY)],
        out_specs=pl.BlockSpec(memory_space=pl.ANY),
        scratch_shapes=[
            pltpu.VMEM((n * n, g, n * parts * w), jnp.bfloat16),
            pltpu.VMEM((slots, g, g), jnp.bfloat16),
            pltpu.VMEM((n, g, n * parts * w), jnp.float32),
            pltpu.VMEM((n * n * 2, parts, g // 2, w), jnp.bfloat16),
            (
                sem((n, parts, n - 1)),
                sem((slots, parts)),
                sem((slots, parts)),
                sem((slots, parts)),
                sem((slots, n)),
                sem((slots, sends)),
                sem((slots, n)),
                sem,
                sem((n * n * 2,)),
            ),
        ],
        compiler_params=pltpu.CompilerParams(
            has_side_effects=True, vmem_limit_bytes=60 * 2**20
        ),
    )(inverse_factor)
    first_row = (lax.axis_index("row") * n_col + lax.axis_index("col")) * (order // (n * n_col))
    own_alpha = lax.dynamic_slice_in_dim(alpha_vector, first_row, order // (n * n_col), 0)
    return pl.pallas_call(
        functools.partial(output_kernel, scale),
        out_shape=jax.ShapeDtypeStruct((g // 2, order), jnp.float32),
        grid=(n,),
        in_specs=[
            pl.BlockSpec((n, g // 2, g), lambda i: (i, 0, 0)),
            pl.BlockSpec((g // 2, 1), lambda i: (0, 0)),
            pl.BlockSpec((1, n * g), lambda i: (0, i)),
        ],
        out_specs=pl.BlockSpec((g // 2, n * g), lambda i: (0, i)),
    )(coded, own_alpha[:, None], alpha_vector[None, :])


def layers(inverse_factor, alpha_vector):
    layer = lax.axis_index("row")
    column = lax.axis_index("col")
    n_row = lax.axis_size("row")
    n_col = lax.axis_size("col")
    tile_rows, tile_cols = inverse_factor.shape
    ratio = n_col // n_row
    width = tile_cols // n_row
    gathered = lax.all_gather(inverse_factor, "col", axis=0, tiled=False)
    block_in_layer = column * width // tile_cols
    first_col = column * width % tile_cols

    def owned_by(dest):
        start = (dest * ratio + block_in_layer, 0, first_col)
        return lax.dynamic_slice(gathered, start, (1, tile_rows, width))[0]

    sides = (n_row // square_side(n_row), square_side(n_row))
    place = (layer // sides[1], layer % sides[1])

    def index(first, second, order):
        return second * sides[1] + first if order else first * sides[1] + second

    def reduced(block, order):
        chunk = block // ratio
        n_first, n_second = (sides[1], sides[0]) if order else sides
        first, second = (place[1], place[0]) if order else place

        def dest(u, v, s, t):
            return index((u - s) % n_first, (v - t) % n_second, order)

        def partial_of(s, t):
            left = owned_by(dest(first, second, s, t))
            return contract(left, gathered[block])

        def owes(u, v, s, t):
            g = index(u, v, order)
            return g >= chunk and g >= dest(u, v, s, t)

        places = [(u, v) for u in range(n_first) for v in range(n_second)]

        def first_hop(s, t):
            pairs = [
                (index(u, v, order), dest(u, v, s, 0)) for u, v in places if owes(u, v, s, t)
            ]
            if not pairs:
                return None
            return lax.ppermute(partial_of(s, t).astype(jnp.float16), "row", pairs)

        def second_hop(value, t):
            pairs = []
            for u, v in places:
                if any(owes((u + s) % n_first, v, s, t) for s in range(n_first)):
                    pairs.append((index(u, v, order), dest(u, v, 0, t)))
            if not pairs:
                return None
            return lax.ppermute(value.astype(jnp.float16), "row", pairs)

        def add(total, part):
            return total if part is None else total + part.astype(jnp.float32)

        hops = {}
        for t in range(n_second - 1, -1, -1):
            for s in range(n_first - 1, 0, -1):
                hops[s, t] = first_hop(s, t)

        def finish():
            parts = []
            for t in range(n_second - 1, 0, -1):
                value = partial_of(0, t)
                for s in range(1, n_first):
                    value = add(value, hops[s, t])
                parts.append(second_hop(value, t))
            total = partial_of(0, 0)
            for s in range(1, n_first):
                total = add(total, hops[s, 0])
            for part in parts:
                total = add(total, part)
            return total

        return finish

    first_row = (layer * n_col + column) * width
    own_alpha = lax.dynamic_slice_in_dim(alpha_vector, first_row, width, 0)
    pieces = []
    for finish in [reduced(block, block % 2) for block in range(n_col)]:
        alpha = lax.slice_in_dim(
            alpha_vector, len(pieces) * tile_cols, (len(pieces) + 1) * tile_cols
        )
        pieces.append(finish() - own_alpha[:, None] * alpha[None, :])
    return jnp.concatenate(pieces, axis=1)


def per_device(inverse_factor, alpha_vector):
    n_row, n_col = lax.axis_size("row"), lax.axis_size("col")
    aligned = inverse_factor.shape[0] % (n_row * n_row * LANES) == 0
    if n_col == 2 * n_row and n_row % 2 == 0 and aligned:
        return planes(inverse_factor, alpha_vector)
    return layers(inverse_factor, alpha_vector)


def solution(mesh):
    in_specs = (P("row", "col"), P())
    out_specs = P(("row", "col"), None)
    return jax.shard_map(
        per_device, mesh=mesh, in_specs=in_specs, out_specs=out_specs, check_vma=False
    )
```

```python
import functools

import jax
import jax.numpy as jnp
from jax import lax
from jax.experimental import pallas as pl
from jax.experimental.pallas import tpu as pltpu
from jax.sharding import PartitionSpec as P

LANES = 128
MESH = pl.DeviceIdType.MESH
OFFSET = 2.0**-10
SCATTER_AHEAD = 16
OWN_AHEAD = 1
SKEW = (2, 5, 7)
EDGE_SKEW = (1, 3, 5)


def contract(left, right):
    return lax.dot_general(
        left, right, (((0,), (0,)), ((), ())), preferred_element_type=jnp.float32
    )


def square_side(count):
    return max(side for side in range(1, count + 1) if count % side == 0 and side * side <= count)


def code_scale(order):
    scale = 1.0
    while 4 * order * scale > 2**15:
        scale /= 2
    return scale


def encode(value, scale):
    base = jnp.abs(value) * scale + OFFSET
    base = base * base
    base = base * base
    base = base * base - OFFSET**8
    return jnp.where(value < 0, -base, base).astype(jnp.bfloat16)


def decode(code, scale):
    code = code.astype(jnp.float32)
    power = jnp.abs(code) + OFFSET**8
    fourth = lax.rsqrt(lax.rsqrt(power))
    root = fourth * lax.rsqrt(fourth) - OFFSET
    return jnp.where(code < 0, -root, root) * (1.0 / scale)


def output_kernel(scale, code_ref, own_ref, alpha_ref, out_ref):
    width = code_ref.shape[2]
    for i in range(code_ref.shape[0]):
        at = slice(i * width, (i + 1) * width)
        out_ref[:, at] = decode(code_ref[i], scale) - own_ref[...] * alpha_ref[:, at]


def gram_kernel(n, scale, x_ref, out_ref, cols, rows, acc, coded, sems):
    (x_send, z_recv, right_send, left_send, r_recv, r_send, d_send, o_recv, o_send) = sems
    s = lax.axis_index("row")
    c = lax.axis_index("col")
    z, h = lax.div(c, 2), lax.rem(c, 2)
    parts = n // 2
    g = x_ref.shape[0] // n
    w = g // n
    steps = n * n
    side = n // square_side(n), square_side(n)
    s_hi, s_lo = lax.div(s, side[1]), lax.rem(s, side[1])
    row_core, row_part = lax.div(z, parts), lax.rem(z, parts)
    on_row_core = h == row_core
    lo_peers = [s_hi * side[1] + lax.rem(s_lo + i, side[1]) for i in range(1, side[1])]
    hi_peers = [lax.rem(s_hi + i, side[0]) * side[1] + s_lo for i in range(1, side[0])]

    def slot(f, b):
        k, j = lax.div(f, n), lax.rem(f, n)
        return (lax.div(k * (k + 1), 2) + b) * n + j

    def lanes(index, width):
        return pl.ds(pl.multiple_of(index * width, LANES), width)

    def col_group(b, p):
        return n * b + parts * h + p

    def exists(f, b, p):
        return (b >= 0) & (b < n) & (col_group(b, p) <= f)

    def col_piece(f, b, p):
        return cols.at[f, :, lanes(b * parts + p, w)]

    def row_piece(f, a, origin):
        return rows.at[slot(f, a), :, lanes(origin, w)]

    def remote(src, dst, send, recv, row, col):
        return pltpu.make_async_remote_copy(
            src_ref=src, dst_ref=dst, send_sem=send, recv_sem=recv,
            device_id=(row, col), device_id_type=MESH,
        )

    def scatter(f, act):
        j = lax.rem(f, n)
        for p in range(parts):

            @pl.when((lax.div(f, n) == s) & exists(f, z, p))
            def _():
                for i in range(n):
                    dest = lax.rem(s + i, n)
                    src = x_ref.at[
                        pl.ds(pl.multiple_of(j * g, g), g),
                        pl.ds(pl.multiple_of(p * g + dest * w, LANES), w),
                    ]
                    sem = z_recv.at[slot(f, z), p]
                    if i > 0:
                        copy = remote(src, col_piece(f, z, p), x_send.at[j, p, i - 1], sem, dest, c)
                        copy.start() if act == "start" else copy.wait_send()
                    elif act == "start":
                        pltpu.make_async_copy(src, col_piece(f, z, p), sem).start()

    def z_copy(f, b, p, step):
        send = right_send if step > 0 else left_send
        piece = col_piece(f, b, p)
        return remote(piece, piece, send.at[slot(f, b), p], z_recv.at[slot(f, b), p], s, c + 2 * step)

    def z_wait(f, b, p):
        piece = col_piece(f, b, p)
        pltpu.make_async_copy(piece, piece, z_recv.at[slot(f, b), p]).wait()

    def r_copy(f, a, origin, row, index, src=None):
        piece = row_piece(f, a, origin)
        return remote(
            piece if src is None else src, piece, r_send.at[slot(f, a), index],
            r_recv.at[slot(f, a), origin], row, c,
        )

    def d_copy(f, a, origin, src=None):
        piece = row_piece(f, a, origin)
        return remote(
            piece if src is None else src, piece, d_send.at[slot(f, a), origin],
            r_recv.at[slot(f, a), origin], s, c + 1 - 2 * h,
        )

    def r_wait(f, a, origin):
        piece = row_piece(f, a, origin)
        pltpu.make_async_copy(piece, piece, r_recv.at[slot(f, a), origin]).wait()

    def by_order(turn, action):
        @pl.when(lax.rem(turn, 2) == 0)
        def _():
            action(lo_peers, hi_peers)

        @pl.when(lax.rem(turn, 2) == 1)
        def _():
            action(hi_peers, lo_peers)

    def own_rows(f, a, p, act):
        src = col_piece(f, a, p)
        copies = [r_copy(f, a, s, peer, i, src) for i, peer in enumerate(lo_peers + hi_peers)]
        copies.append(d_copy(f, a, s, src))
        for copy in copies:
            copy.start() if act == "start" else copy.wait_send()
        if act == "start":
            rows[slot(f, a), :, lanes(s, w)] = cols[f, :, lanes(a * parts + p, w)]

    own_count = len(lo_peers) + len(hi_peers)

    def relay_rows(f, a, act):
        def action(first, second):
            index = own_count
            for origin in first:
                if act == "start":
                    r_wait(f, a, origin)
                copies = []
                for peer in second:
                    copies.append(r_copy(f, a, origin, peer, index))
                    index += 1
                copies.append(d_copy(f, a, origin))
                for copy in copies:
                    copy.start() if act == "start" else copy.wait_send()

        by_order(f + a, action)

    def last_rows(f, a, act):
        def full(first, second, first_is_lo):
            for i in range(len(second)):
                origins = [second[i]]
                for m in range(len(first)):
                    if first_is_lo:
                        hi = lax.div(second[i], side[1])
                        lo = lax.rem(first[m], side[1])
                    else:
                        hi = lax.div(first[m], side[1])
                        lo = lax.rem(second[i], side[1])
                    origins.append(hi * side[1] + lo)
                for origin in origins:
                    if act == "start":
                        r_wait(f, a, origin)
                    copy = d_copy(f, a, origin)
                    copy.start() if act == "start" else copy.wait_send()

        @pl.when(lax.rem(f + a, 2) == 0)
        def _():
            full(lo_peers, hi_peers, True)

        @pl.when(lax.rem(f + a, 2) == 1)
        def _():
            full(hi_peers, lo_peers, False)

    def pass_on(f, b, p, act, wait):
        if act == "start" and wait:
            z_wait(f, b, p)

        @pl.when((b <= z) & (z < n - 1))
        def _():
            copy = z_copy(f, b, p, 1)
            copy.start() if act == "start" else copy.wait_send()

        @pl.when((b >= z) & (z > 0))
        def _():
            copy = z_copy(f, b, p, -1)
            copy.start() if act == "start" else copy.wait_send()

        @pl.when(on_row_core & (row_part == p))
        def _():
            own_rows(f, b, p, act)

    def own_columns(f, act):
        for p in range(parts):

            @pl.when(exists(f, z, p))
            def _():
                pass_on(f, z, p, act, True)

    def other_columns(f, act):
        for distance in range(1, n):
            for b in (z - distance, z + distance):
                for p in range(parts):

                    @pl.when(exists(f, b, p))
                    def _():
                        pass_on(f, b, p, act, True)

    def row_blocks(f):
        k, j = lax.div(f, n), lax.rem(f, n)
        return k + (z <= j).astype(jnp.int32)

    def col_blocks(f):
        k, j = lax.div(f, n), lax.rem(f, n)
        return k + (parts * h <= j).astype(jnp.int32)

    def each_row_block(f, action):
        @pl.when(on_row_core)
        def _():
            @pl.loop(0, row_blocks(f))
            def _(a):
                action(a)

    def compute(f):
        @pl.when(~on_row_core)
        def _():
            @pl.loop(0, row_blocks(f))
            def _(a):
                for origin in range(n):
                    r_wait(f, a, origin)

        @pl.loop(0, row_blocks(f))
        def _(a):
            for blocks in range(1, n + 1):

                @pl.when(col_blocks(f) == blocks)
                def _():
                    width = blocks * parts * w
                    acc[a, :, :width] += contract(rows[slot(f, a)], cols[f, :, :width])

    def result_copies(a, b, act):
        for half in range(2):
            index = (a * n + b) * 2 + half
            src = coded.at[index]
            dst = out_ref.at[pl.ds((2 * b + h) * parts, parts), :, lanes(s, w)]
            owner = 2 * z + half
            here = (a == s) & (half == h)

            @pl.when(here)
            def _():
                if act == "start":
                    pltpu.make_async_copy(src, dst, o_recv).start()

            @pl.when(~here)
            def _():
                copy = remote(src, dst, o_send.at[index], o_recv, a, owner)
                copy.start() if act == "start" else copy.wait_send()

    def result(a, b):
        for half in range(2):
            for p in range(parts):
                value = acc[a, half * (g // 2):(half + 1) * (g // 2), lanes(b * parts + p, w)]
                coded[(a * n + b) * 2 + half, p] = encode(value, scale)
        result_copies(a, b, "start")

    def finish(f):
        k = lax.div(f, n)

        @pl.when(lax.rem(f, n) == 0)
        def _():
            @pl.loop(0, k + 1)
            def _(i):
                result(k, i)

            @pl.loop(0, k)
            def _(i):
                result(i, k)

    def guarded(f, action):
        @pl.when((f >= 0) & (f < steps))
        def _():
            action(f)

    for i in range(SCATTER_AHEAD):
        scatter(jnp.int32(steps - 1 - i), "start")

    for j in range(n):
        for p in range(parts):

            @pl.when((j >= parts * h) & (j < parts * h + p))
            def _():
                @pl.loop(0, n)
                def _(k):
                    cols[n * k + j, :, lanes(k * parts + p, w)] = jnp.zeros((g, w), cols.dtype)

    @pl.loop(0, n)
    def _(i):
        acc[i] = jnp.zeros(acc.shape[1:], acc.dtype)

    for i in range(OWN_AHEAD):
        own_columns(jnp.int32(steps - 1 - i), "start")

    @pl.when(z == 0)
    def _():
        own_columns(jnp.int32(steps - 1 - OWN_AHEAD), "start")

    behind = [jnp.where(z == n - 1, edge, inner) for edge, inner in zip(EDGE_SKEW, SKEW)]

    @pl.loop(0, steps + SKEW[2])
    def _(t):
        f = steps - 1 - t
        guarded(f - SCATTER_AHEAD, lambda f: scatter(f, "start"))

        @pl.when(z == 0)
        def _():
            guarded(f - OWN_AHEAD - 1, lambda f: own_columns(f, "start"))

        guarded(f, lambda f: other_columns(f, "start"))

        @pl.when(~(z == 0))
        def _():
            guarded(f - OWN_AHEAD, lambda f: own_columns(f, "start"))

        guarded(f + behind[0], lambda f: each_row_block(f, lambda a: relay_rows(f, a, "start")))
        guarded(f + behind[1], lambda f: each_row_block(f, lambda a: last_rows(f, a, "start")))

        def last(f):
            compute(f)
            finish(f)

        guarded(f + behind[2], last)

    @pl.loop(0, steps)
    def _(f):
        scatter(f, "wait")
        own_columns(f, "wait")
        other_columns(f, "wait")
        each_row_block(f, lambda a: relay_rows(f, a, "wait"))
        each_row_block(f, lambda a: last_rows(f, a, "wait"))

    @pl.loop(0, n)
    def _(a):
        @pl.loop(0, n)
        def _(b):
            result_copies(a, b, "wait")

    pltpu.make_async_copy(out_ref, out_ref, o_recv).wait()


def planes(inverse_factor, alpha_vector):
    n = lax.axis_size("row")
    n_col = lax.axis_size("col")
    tile_rows, tile_cols = inverse_factor.shape
    order = alpha_vector.shape[0]
    parts, g = n // 2, tile_rows // n
    w = g // n
    scale = code_scale(order)
    slots = n * (n + 1) // 2 * n
    sem = pltpu.SemaphoreType.DMA
    side = n // square_side(n), square_side(n)
    sends = (side[0] - 1) + (side[1] - 1) + (side[0] - 1) * (side[1] - 1)
    coded = pl.pallas_call(
        functools.partial(gram_kernel, n, scale),
        out_shape=jax.ShapeDtypeStruct((n * n, g // 2, n * w), jnp.bfloat16),
        in_specs=[pl.BlockSpec(memory_space=pl.ANY)],
        out_specs=pl.BlockSpec(memory_space=pl.ANY),
        scratch_shapes=[
            pltpu.VMEM((n * n, g, n * parts * w), jnp.bfloat16),
            pltpu.VMEM((slots, g, g), jnp.bfloat16),
            pltpu.VMEM((n, g, n * parts * w), jnp.float32),
            pltpu.VMEM((n * n * 2, parts, g // 2, w), jnp.bfloat16),
            (
                sem((n, parts, n - 1)),
                sem((slots, parts)),
                sem((slots, parts)),
                sem((slots, parts)),
                sem((slots, n)),
                sem((slots, sends)),
                sem((slots, n)),
                sem,
                sem((n * n * 2,)),
            ),
        ],
        compiler_params=pltpu.CompilerParams(
            has_side_effects=True, vmem_limit_bytes=60 * 2**20
        ),
    )(inverse_factor)
    first_row = (lax.axis_index("row") * n_col + lax.axis_index("col")) * (order // (n * n_col))
    own_alpha = lax.dynamic_slice_in_dim(alpha_vector, first_row, order // (n * n_col), 0)
    return pl.pallas_call(
        functools.partial(output_kernel, scale),
        out_shape=jax.ShapeDtypeStruct((g // 2, order), jnp.float32),
        grid=(n,),
        in_specs=[
            pl.BlockSpec((n, g // 2, g), lambda i: (i, 0, 0)),
            pl.BlockSpec((g // 2, 1), lambda i: (0, 0)),
            pl.BlockSpec((1, n * g), lambda i: (0, i)),
        ],
        out_specs=pl.BlockSpec((g // 2, n * g), lambda i: (0, i)),
    )(coded, own_alpha[:, None], alpha_vector[None, :])


def layers(inverse_factor, alpha_vector):
    layer = lax.axis_index("row")
    column = lax.axis_index("col")
    n_row = lax.axis_size("row")
    n_col = lax.axis_size("col")
    tile_rows, tile_cols = inverse_factor.shape
    ratio = n_col // n_row
    width = tile_cols // n_row
    gathered = lax.all_gather(inverse_factor, "col", axis=0, tiled=False)
    block_in_layer = column * width // tile_cols
    first_col = column * width % tile_cols

    def owned_by(dest):
        start = (dest * ratio + block_in_layer, 0, first_col)
        return lax.dynamic_slice(gathered, start, (1, tile_rows, width))[0]

    sides = (n_row // square_side(n_row), square_side(n_row))
    place = (layer // sides[1], layer % sides[1])

    def index(first, second, order):
        return second * sides[1] + first if order else first * sides[1] + second

    def reduced(block, order):
        chunk = block // ratio
        n_first, n_second = (sides[1], sides[0]) if order else sides
        first, second = (place[1], place[0]) if order else place

        def dest(u, v, s, t):
            return index((u - s) % n_first, (v - t) % n_second, order)

        def partial_of(s, t):
            left = owned_by(dest(first, second, s, t))
            return contract(left, gathered[block])

        def owes(u, v, s, t):
            g = index(u, v, order)
            return g >= chunk and g >= dest(u, v, s, t)

        places = [(u, v) for u in range(n_first) for v in range(n_second)]

        def first_hop(s, t):
            pairs = [
                (index(u, v, order), dest(u, v, s, 0)) for u, v in places if owes(u, v, s, t)
            ]
            if not pairs:
                return None
            return lax.ppermute(partial_of(s, t).astype(jnp.float16), "row", pairs)

        def second_hop(value, t):
            pairs = []
            for u, v in places:
                if any(owes((u + s) % n_first, v, s, t) for s in range(n_first)):
                    pairs.append((index(u, v, order), dest(u, v, 0, t)))
            if not pairs:
                return None
            return lax.ppermute(value.astype(jnp.float16), "row", pairs)

        def add(total, part):
            return total if part is None else total + part.astype(jnp.float32)

        hops = {}
        for t in range(n_second - 1, -1, -1):
            for s in range(n_first - 1, 0, -1):
                hops[s, t] = first_hop(s, t)

        def finish():
            parts = []
            for t in range(n_second - 1, 0, -1):
                value = partial_of(0, t)
                for s in range(1, n_first):
                    value = add(value, hops[s, t])
                parts.append(second_hop(value, t))
            total = partial_of(0, 0)
            for s in range(1, n_first):
                total = add(total, hops[s, 0])
            for part in parts:
                total = add(total, part)
            return total

        return finish

    first_row = (layer * n_col + column) * width
    own_alpha = lax.dynamic_slice_in_dim(alpha_vector, first_row, width, 0)
    pieces = []
    for finish in [reduced(block, block % 2) for block in range(n_col)]:
        alpha = lax.slice_in_dim(
            alpha_vector, len(pieces) * tile_cols, (len(pieces) + 1) * tile_cols
        )
        pieces.append(finish() - own_alpha[:, None] * alpha[None, :])
    return jnp.concatenate(pieces, axis=1)


def per_device(inverse_factor, alpha_vector):
    n_row, n_col = lax.axis_size("row"), lax.axis_size("col")
    aligned = inverse_factor.shape[0] % (n_row * n_row * LANES) == 0
    if n_col == 2 * n_row and n_row % 2 == 0 and aligned:
        return planes(inverse_factor, alpha_vector)
    return layers(inverse_factor, alpha_vector)


def solution(mesh):
    in_specs = (P("row", "col"), P())
    out_specs = P(("row", "col"), None)
    return jax.shard_map(
        per_device, mesh=mesh, in_specs=in_specs, out_specs=out_specs, check_vma=False
    )
```
